32 devices in a mesh: tm: 4 (over x, core), batch: 8 (over z, y).
Axes of the slice: x: 2, y: 2, z: 4, core: 2. Of those that a mesh axis runs over, the one named last changes fastest.
Arguments:
- initial_state: float32 [2048, 256], P('batch'), may hold values from -6 to 6
- increments: float32 [32, 2048, 256], P('tm', 'batch'), may hold values from -1.5 to 1.5
- cotangents: float32 [32, 2048, 256], P('tm', 'batch'), may hold values from -1.5 to 1.5
- drift_inner: bfloat16 [256, 1024], replicated, may hold values from -0.375 to 0.375
- drift_hidden: float32 [1024], replicated, may hold values from -3 to 3
- drift_outer: bfloat16 [1024, 256], replicated, may hold values from -0.1875 to 0.1875
- drift_offset: float32 [256], replicated, may hold values from -3 to 3
- noise_inner: bfloat16 [256, 1024], replicated, may hold values from -0.375 to 0.375
- noise_hidden: float32 [1024], replicated, may hold values from -3 to 3
- noise_outer: bfloat16 [1024, 256], replicated, may hold values from -0.1875 to 0.1875
- noise_offset: float32 [256], replicated, may hold values from -4 to 4
Outputs:
- states: float32 [32, 2048, 256], P('tm', 'batch')
- adjoints: float32 [32, 2048, 256], P('tm', 'batch')
- drift_inner_grad: float32 [256, 1024], replicated
- drift_hidden_grad: float32 [1024], replicated
- drift_outer_grad: float32 [1024, 256], replicated
- drift_offset_grad: float32 [256], replicated
- noise_inner_grad: float32 [256, 1024], replicated
- noise_hidden_grad: float32 [1024], replicated
- noise_outer_grad: float32 [1024, 256], replicated
- noise_offset_grad: float32 [256], replicated
The draws below stay inside these ranges and needn't reach their ends.
All inputs are finite; a program needn't handle non-finite values.
Results may differ from the reference program's by a relative error of at most 0.0095.
Values sent between devices are 32-bit elements; how exact they have to be, the bound alone decides.
No kernel may reach another device: no remote copies, remote signals or barrier semaphores. Data moves between devices by JAX's collectives and lax.ppermute only.
A program may use at most 128 MiB of HBM per device.

```python
import math
import jax
import jax.numpy as jnp
from jax import lax

L = 256
H = 1024
STEPS = 32
BATCH = 2048


def block_scale(own_key, shape, pieces, smallest, largest):
    def one(dim, blocks):
        draws = jax.random.uniform(jax.random.fold_in(jax.random.fold_in(own_key, 6), dim), (blocks,), jnp.float32, smallest / len(pieces), largest / len(pieces))
        return jnp.repeat(jnp.exp(draws), shape[dim] // blocks).reshape((-1,) + (1,) * (len(shape) - dim - 1))

    loudness = one(*pieces[0])
    for cut in pieces[1:]:
        loudness = loudness * one(*cut)
    return loudness


def scatter_about(stream_key, dims, deviation, most, pieces=(), held_as=jnp.bfloat16):
    array = jax.random.normal(stream_key, dims, jnp.float32) * deviation
    if len(pieces) > 0:
        array = block_scale(stream_key, dims, pieces, -0.22, 0.18) * array
    return jnp.clip(array, min=-most, max=most).astype(held_as)


def setup_inputs(seed: int = 0) -> dict:
    seeds = jax.random.split(jax.random.key(seed), 12)
    initial_state = scatter_about(seeds[0], (BATCH, L), 1.0, 6.0, ((0, 8),), jnp.float32)
    increments = scatter_about(seeds[1], (STEPS, BATCH, L), 0.224, 1.5, ((0, 4), (1, 8)), jnp.float32)
    cotangents = scatter_about(seeds[2], (STEPS, BATCH, L), 0.25, 1.5, ((0, 4), (1, 8)), jnp.float32)
    drift_inner = scatter_about(seeds[3], (L, H), L ** -0.5, 0.375)
    drift_hidden = scatter_about(seeds[4], (H,), 0.5, 3.0, (), jnp.float32)
    drift_outer = scatter_about(seeds[5], (H, L), H ** -0.5, 0.1875)
    drift_offset = scatter_about(seeds[6], (L,), 0.5, 3.0, (), jnp.float32)
    noise_inner = scatter_about(seeds[7], (L, H), L ** -0.5, 0.375)
    noise_hidden = scatter_about(seeds[8], (H,), 0.5, 3.0, (), jnp.float32)
    noise_outer = scatter_about(seeds[9], (H, L), H ** -0.5, 0.1875)
    noise_offset = scatter_about(seeds[10], (L,), 1.0, 4.0, (), jnp.float32)
    return {"initial_state": initial_state, "increments": increments, "cotangents": cotangents, "drift_inner": drift_inner, "drift_hidden": drift_hidden, "drift_outer": drift_outer, "drift_offset": drift_offset, "noise_inner": noise_inner, "noise_hidden": noise_hidden, "noise_outer": noise_outer, "noise_offset": noise_offset}


delta_time = 0.05

def matmul(left, right):
    return jnp.dot(left, right, preferred_element_type=jnp.float32)

def matmul_transposed(left, right):
    return lax.dot_general(left, right, (((1,), (1,)), ((), ())), preferred_element_type=jnp.float32)

def matmul_rows(left, right):
    return lax.dot_general(left, right, (((0,), (0,)), ((), ())), preferred_element_type=jnp.float32)

def advance(state, noise, params):
    drift_inner, drift_hidden, drift_outer, drift_offset, noise_inner, noise_hidden, noise_outer, noise_offset = params
    state_low = state.astype(jnp.bfloat16)
    hidden_drift = jnp.tanh(matmul(state_low, drift_inner) + drift_hidden).astype(jnp.bfloat16)
    hidden_noise = jnp.tanh(matmul(state_low, noise_inner) + noise_hidden).astype(jnp.bfloat16)
    drift = matmul(hidden_drift, drift_outer) + drift_offset
    spread = jax.nn.sigmoid(matmul(hidden_noise, noise_outer) + noise_offset)
    return (state + delta_time * drift + spread * noise, (state_low, hidden_drift, hidden_noise, spread))

def retreat(adjoint_next, state, noise, params):
    drift_inner, drift_hidden, drift_outer, drift_offset, noise_inner, noise_hidden, noise_outer, noise_offset = params
    unused, saved = advance(state, noise, params)
    state_low, hidden_drift, hidden_noise, spread = saved
    drift_grad = delta_time * adjoint_next
    noise_grad = adjoint_next * noise * spread * (1.0 - spread)
    drift_low = drift_grad.astype(jnp.bfloat16)
    noise_low = noise_grad.astype(jnp.bfloat16)
    back_drift = matmul_transposed(drift_low, drift_outer) * (1.0 - jnp.square(hidden_drift.astype(jnp.float32)))
    back_noise = matmul_transposed(noise_low, noise_outer) * (1.0 - jnp.square(hidden_noise.astype(jnp.float32)))
    back_drift_low = back_drift.astype(jnp.bfloat16)
    back_noise_low = back_noise.astype(jnp.bfloat16)
    adjoint = adjoint_next + matmul_transposed(back_drift_low, drift_inner) + matmul_transposed(back_noise_low, noise_inner)
    grads = (matmul_rows(state_low, back_drift_low), lax.optimization_barrier(jnp.sum(back_drift, 0)), matmul_rows(hidden_drift, drift_low), lax.optimization_barrier(jnp.sum(drift_grad, 0)), matmul_rows(state_low, back_noise_low), lax.optimization_barrier(jnp.sum(back_noise, 0)), matmul_rows(hidden_noise, noise_low), lax.optimization_barrier(jnp.sum(noise_grad, 0)))
    return (adjoint, grads)

def squares(grads):
    total = jnp.sum(jnp.square(grads[0]))
    for entry in grads[1:]:
        total = total + jnp.sum(jnp.square(entry))
    return total

def clip_factor(total):
    limit = 0.5 * math.sqrt(4 * L * H + 2 * H + 2 * L)
    return jnp.minimum(1.0, limit / jnp.sqrt(total))

def reference(initial_state, increments, cotangents, drift_inner, drift_hidden, drift_outer, drift_offset, noise_inner, noise_hidden, noise_outer, noise_offset):
    params = (drift_inner, drift_hidden, drift_outer, drift_offset, noise_inner, noise_hidden, noise_outer, noise_offset)

    def forward(state, noise):
        following, unused = advance(state, noise, params)
        return (following, (state, following))
    final, (entries, states) = lax.scan(forward, initial_state, increments)
    blank = tuple((jnp.zeros(p.shape, jnp.float32) for p in params))

    def backward(carry, inputs):
        adjoint_next, totals = carry
        entry, noise, cotangent = inputs
        adjoint, grads = retreat(adjoint_next + cotangent, entry, noise, params)
        totals = tuple((a + b for a, b in zip(totals, grads)))
        return ((adjoint, totals), adjoint)
    (unused, totals), adjoints = lax.scan(backward, (jnp.zeros_like(initial_state), blank), (entries, increments, cotangents), reverse=True)
    factor = clip_factor(squares(totals))
    return (states, adjoints, totals[0] * factor, totals[1] * factor, totals[2] * factor, totals[3] * factor, totals[4] * factor, totals[5] * factor, totals[6] * factor, totals[7] * factor)
```

```python
import functools
import math

import jax
import jax.numpy as jnp
from jax import lax
from jax.experimental import pallas as pl
from jax.experimental.pallas import tpu as pltpu
from jax.sharding import PartitionSpec as P

delta_time = 0.05
TILE = 256
LANES = 128
COLORS = 3
PARAMS = pltpu.CompilerParams(vmem_limit_bytes=60 * 1024 * 1024)
ANY = pl.BlockSpec(memory_space=pl.ANY)
VMEM = pl.BlockSpec(memory_space=pltpu.VMEM)
SMEM = pl.BlockSpec(memory_space=pltpu.SMEM)


def dot(left, right):
    return jnp.dot(left, right, preferred_element_type=jnp.float32)


def dot_rows(left, right):
    return lax.dot_general(
        left, right, (((0,), (0,)), ((), ())), preferred_element_type=jnp.float32
    )


def step_copies(own, received, core, half, rows, steps, buffer, sems, k):
    local = lax.rem(k, steps)
    from_own = pltpu.make_async_copy(
        own.at[local, pl.ds(pl.multiple_of(core * rows, 8), rows), :], buffer.at[k], sems.at[k]
    )
    from_mate = pltpu.make_async_copy(received.at[local], buffer.at[k], sems.at[k])
    return from_own, from_mate


def forward_kernel(
    full,
    steps,
    rows,
    info,
    initial,
    incoming,
    own_noise,
    mate_noise,
    drift_inner,
    drift_hidden,
    drift_outer,
    drift_offset,
    noise_inner,
    noise_hidden,
    noise_outer,
    noise_offset,
    *rest,
):
    if full:
        final, states, states_send, q_out, u_out, v_out, a_out = rest[:7]
        noise_buf, in_sems, out_sem, z_buf, q_buf, u_buf, v_buf, a_buf = rest[7:]
    else:
        final, noise_buf, in_sems = rest
    window = 2 * steps
    core = info[0]
    first = info[1]
    hidden = drift_inner.shape[1]

    def start(k, carry):
        mine = k // steps == core
        from_own, from_mate = step_copies(
            own_noise, mate_noise, core, None, rows, steps, noise_buf, in_sems, k
        )

        @pl.when(mine)
        def _():
            from_own.start()

        @pl.when(jnp.logical_not(mine))
        def _():
            from_mate.start()

        return carry

    lax.fori_loop(0, window, start, 0)
    begin = jnp.where(first == 1, initial[pl.ds(pl.multiple_of(core * rows, 8), rows), :], incoming[...])

    def state_copies(k):
        local = lax.rem(k, steps)
        keep = pltpu.make_async_copy(
            z_buf.at[k],
            states.at[local, pl.ds(pl.multiple_of(core * rows, 8), rows), :],
            out_sem,
        )
        send = pltpu.make_async_copy(z_buf.at[k], states_send.at[local], out_sem)
        return keep, send

    def saved_copies(k):
        return [
            pltpu.make_async_copy(buf.at[k], out.at[k], out_sem)
            for buf, out in ((q_buf, q_out), (u_buf, u_out), (v_buf, v_out), (a_buf, a_out))
        ]

    def body(k, state):
        pltpu.make_async_copy(mate_noise.at[0], noise_buf.at[k], in_sems.at[k]).wait()
        q = state.astype(jnp.bfloat16)
        if full:
            q_buf[k] = q
        drift = drift_offset[...]
        spread = noise_offset[...]
        for j in range(hidden // TILE):
            cols = slice(j * TILE, (j + 1) * TILE)
            u = jnp.tanh(dot(q, drift_inner[:, cols]) + drift_hidden[:, cols]).astype(jnp.bfloat16)
            v = jnp.tanh(dot(q, noise_inner[:, cols]) + noise_hidden[:, cols]).astype(jnp.bfloat16)
            if full:
                u_buf[k, :, cols] = u
                v_buf[k, :, cols] = v
            drift = drift + dot(u, drift_outer[cols, :])
            spread = spread + dot(v, noise_outer[cols, :])
        s = 0.5 * jnp.tanh(0.5 * spread) + 0.5
        noise = noise_buf[k]
        following = state + delta_time * drift + s * noise
        if full:
            a_buf[k] = noise * s * (1.0 - s)
            z_buf[k] = following
            mine = k // steps == core
            keep, send = state_copies(k)

            @pl.when(mine)
            def _():
                keep.start()

            @pl.when(jnp.logical_not(mine))
            def _():
                send.start()

            for copy in saved_copies(k):
                copy.start()
        return following

    final[...] = lax.fori_loop(0, window, body, begin)
    if full:

        def finish(k, carry):
            state_copies(k)[1].wait()
            for copy in saved_copies(k):
                copy.wait()
            return carry

        lax.fori_loop(0, window, finish, 0)


def backward_kernel(
    full,
    steps,
    rows,
    blocks,
    block_rows,
    info,
    incoming,
    own_cotangent,
    mate_cotangent,
    q_in,
    u_in,
    v_in,
    a_in,
    drift_inner_t,
    drift_outer_t,
    noise_inner_t,
    noise_outer_t,
    *rest,
):
    if full:
        final, adjoints, adjoints_send, keep_out, send_out = rest[:5]
        (c_buf, u_buf, v_buf, a_buf, in_sems, q_sem, out_sem, q_buf) = rest[5:13]
        (e_buf, pb_buf, rb_buf, fb_buf, gb_buf, p_sum, r_sum, f_sum, g_sum, packed) = rest[13:]
    else:
        final, c_buf, u_buf, v_buf, a_buf, in_sems = rest
    window = 2 * steps
    core = info[0]
    last = info[2]
    width, hidden = drift_outer_t.shape

    def saved_copies(k):
        return [
            pltpu.make_async_copy(src.at[k], buf.at[k], in_sems.at[k])
            for src, buf in ((u_in, u_buf), (v_in, v_buf), (a_in, a_buf))
        ]

    def start(n, carry):
        k = window - 1 - n
        mine = k // steps == core
        from_own, from_mate = step_copies(
            own_cotangent, mate_cotangent, core, None, rows, steps, c_buf, in_sems, k
        )

        @pl.when(mine)
        def _():
            from_own.start()

        @pl.when(jnp.logical_not(mine))
        def _():
            from_mate.start()

        for copy in saved_copies(k):
            copy.start()
        return carry

    lax.fori_loop(0, window, start, 0)
    if full:
        pltpu.make_async_copy(q_in, q_buf, q_sem).start()
        for ref in (p_sum, r_sum, f_sum, g_sum):
            ref[...] = jnp.zeros_like(ref)
    begin = jnp.where(last == 1, jnp.zeros_like(incoming), incoming[...])

    def adjoint_copies(k):
        local = lax.rem(k, steps)
        keep = pltpu.make_async_copy(
            e_buf.at[k],
            adjoints.at[local, pl.ds(pl.multiple_of(core * rows, 8), rows), :],
            out_sem,
        )
        send = pltpu.make_async_copy(e_buf.at[k], adjoints_send.at[local], out_sem)
        return keep, send

    def partial(x):
        return jnp.sum(x.reshape(rows // 8, 8, x.shape[1]), 0)

    def body(n, adjoint):
        k = window - 1 - n
        pltpu.make_async_copy(mate_cotangent.at[0], c_buf.at[k], in_sems.at[k]).wait()
        for copy in saved_copies(k):
            copy.wait()
        w = adjoint + c_buf[k]
        f = delta_time * w
        g = w * a_buf[k]
        fb = f.astype(jnp.bfloat16)
        gb = g.astype(jnp.bfloat16)
        if full:
            fb_buf[k] = fb
            gb_buf[k] = gb
            f_sum[...] += partial(f)
            g_sum[...] += partial(g)
        result = w
        for j in range(hidden // TILE):
            cols = slice(j * TILE, (j + 1) * TILE)
            u = u_buf[k, :, cols].astype(jnp.float32)
            v = v_buf[k, :, cols].astype(jnp.float32)
            p = dot(fb, drift_outer_t[:, cols]) * (1.0 - u * u)
            r = dot(gb, noise_outer_t[:, cols]) * (1.0 - v * v)
            pb = p.astype(jnp.bfloat16)
            rb = r.astype(jnp.bfloat16)
            if full:
                p_sum[:, cols] += partial(p)
                r_sum[:, cols] += partial(r)
                pb_buf[k, :, cols] = pb
                rb_buf[k, :, cols] = rb
            result = result + dot(pb, drift_inner_t[cols, :])
            result = result + dot(rb, noise_inner_t[cols, :])
        if full:
            e_buf[k] = result
            mine = k // steps == core
            keep, send = adjoint_copies(k)

            @pl.when(mine)
            def _():
                keep.start()

            @pl.when(jnp.logical_not(mine))
            def _():
                send.start()

        return result

    final[...] = lax.fori_loop(0, window, body, begin)
    if not full:
        return
    pltpu.make_async_copy(q_in, q_buf, q_sem).wait()
    total = window * rows
    q = q_buf[...].reshape(total, width)
    per_matrix = width * hidden // LANES
    nets = (
        (pb_buf, fb_buf, u_buf, p_sum, f_sum),
        (rb_buf, gb_buf, v_buf, r_sum, g_sum),
    )
    for net, (back_buf, low_buf, hid_buf, hidden_sum, offset_sum) in enumerate(nets):
        low = low_buf[...].reshape(total, width)
        for j in range(hidden // TILE):
            cols = slice(j * TILE, (j + 1) * TILE)
            inner = dot_rows(q, back_buf[:, :, cols].reshape(total, TILE))
            outer = dot_rows(low, hid_buf[:, :, cols].reshape(total, TILE))
            for i in range(TILE // LANES):
                row = (j * (TILE // LANES) + i) * width
                lanes = slice(i * LANES, (i + 1) * LANES)
                packed[net, row : row + width, :] = inner[:, lanes]
                packed[net, per_matrix + row : per_matrix + row + width, :] = outer[:, lanes]
        base = 2 * per_matrix
        hidden_total = jnp.sum(hidden_sum[...], 0, keepdims=True)
        offset_total = jnp.sum(offset_sum[...], 0, keepdims=True)
        packed[net, base:, :] = jnp.zeros((packed.shape[1] - base, LANES), jnp.float32)
        for i in range(hidden // LANES):
            packed[net, base + i : base + i + 1, :] = hidden_total[:, i * LANES : (i + 1) * LANES]
        base += hidden // LANES
        for i in range(width // LANES):
            packed[net, base + i : base + i + 1, :] = offset_total[:, i * LANES : (i + 1) * LANES]

    def grad_copies(out, net):
        copies = []
        for color in range(COLORS):
            me = info[3 + color]
            for s in range(blocks):
                source = (color * blocks + s) * block_rows
                place = color * blocks + ((s ^ (blocks - 1)) ^ me)
                copies.append(
                    pltpu.make_async_copy(
                        packed.at[net, pl.ds(source, block_rows), :],
                        out.at[pl.ds(pl.multiple_of(place * block_rows, 8), block_rows), :],
                        out_sem,
                    )
                )
        return copies

    for copy in grad_copies(send_out, 1 - core) + grad_copies(keep_out, core):
        copy.start()

    def finish(k, carry):
        adjoint_copies(k)[1].wait()
        return carry

    lax.fori_loop(0, window, finish, 0)
    for copy in grad_copies(send_out, 1 - core) + grad_copies(keep_out, core):
        copy.wait()


def finish_kernel(blocks, block_rows, width, hidden, limit, info, *rest):
    pieces = rest[: 4 * COLORS]
    outs = rest[4 * COLORS : 4 * COLORS + 8]
    packed, sem = rest[4 * COLORS + 8 :]
    core = info[0]
    half = blocks // 2
    copies = []
    for color in range(COLORS):
        me = info[3 + color]
        for side in range(2):
            net = core if side == 0 else 1 - core
            for top in range(2):
                piece = pieces[color * 4 + side * 2 + top]
                for p in range(half):
                    s = (top * half + half - 1 - p) ^ me
                    place = (color * blocks + s) * block_rows
                    copies.append(
                        pltpu.make_async_copy(
                            piece.at[pl.ds(p * block_rows, block_rows), :],
                            packed.at[net, pl.ds(pl.multiple_of(place, 8), block_rows), :],
                            sem,
                        )
                    )
    for copy in copies:
        copy.start()
    for copy in copies:
        copy.wait()
    chunk = block_rows * blocks * COLORS // 8
    acc = jnp.zeros((8, LANES), jnp.float32)
    for net in range(2):
        whole = packed[net]
        acc = acc + jnp.sum(jnp.square(whole).reshape(chunk, 8, LANES), 0)
    total = jnp.sum(jnp.sum(acc, 1, keepdims=True), 0, keepdims=True)
    factor = jnp.minimum(1.0, limit / jnp.sqrt(total))
    per_matrix = width * hidden // LANES
    for net in range(2):
        inner, hidden_out, outer, offset_out = outs[net * 4 : net * 4 + 4]
        for j in range(hidden // LANES):
            lanes = slice(j * LANES, (j + 1) * LANES)
            inner[:, lanes] = packed[net, j * width : (j + 1) * width, :] * factor
            row = per_matrix + j * width
            outer[lanes, :] = (packed[net, row : row + width, :] * factor).T
        base = 2 * per_matrix
        for j in range(hidden // LANES):
            hidden_out[:, j * LANES : (j + 1) * LANES] = packed[net, base + j : base + j + 1, :] * factor
        base += hidden // LANES
        for j in range(width // LANES):
            offset_out[:, j * LANES : (j + 1) * LANES] = packed[net, base + j : base + j + 1, :] * factor


def flipped(block, axis, bit):
    return lax.ppermute(block, axis, [(i, i ^ bit) for i in range(lax.axis_size(axis))])


def moved(block, distance):
    count = lax.axis_size("tm")
    return lax.ppermute(
        block, "tm", [(i, i + distance) for i in range(count) if 0 <= i + distance < count]
    )


def bits_of(size):
    return [1 << i for i in range(size.bit_length() - 1)]


def shards(
    initial_state,
    increments,
    cotangents,
    drift_inner,
    drift_hidden,
    drift_outer,
    drift_offset,
    noise_inner,
    noise_hidden,
    noise_outer,
    noise_offset,
):
    f32, bf16 = jnp.float32, jnp.bfloat16
    segments = lax.axis_size("tm")
    segment = lax.axis_index("tm")
    group = lax.axis_index("batch")
    core = segment % 2
    stages = segments // 2
    stage = segment // 2
    steps, local_rows, width = increments.shape
    hidden = drift_inner.shape[1]
    rows = local_rows // 2
    window = 2 * steps

    dims = [("tm", bit) for bit in bits_of(segments)[1:]]
    dims += [("batch", bit) for bit in bits_of(lax.axis_size("batch"))]
    turn = min(COLORS, len(dims))
    orders = [dims[i % turn : turn] + dims[: i % turn] + dims[turn:] for i in range(COLORS)]
    blocks = 1 << len(dims)
    used = (2 * width * hidden + hidden + width) // LANES
    block_rows = 8 * (-(-used // (8 * blocks * COLORS)))
    color_rows = blocks * block_rows
    packed_rows = COLORS * color_rows

    def position(order):
        place = jnp.int32(0)
        for axis, bit in order:
            index = segment if axis == "tm" else group
            place = 2 * place + (index // bit) % 2
        return place

    info = jnp.stack(
        [core, (stage == 0).astype(jnp.int32), (stage == stages - 1).astype(jnp.int32)]
        + [position(order) for order in orders]
    ).astype(jnp.int32)

    def other_half(array):
        return lax.dynamic_slice_in_dim(array, (1 - core) * rows, rows, 1)

    mate_noise = flipped(other_half(increments), "tm", 1)
    mate_cotangent = flipped(other_half(cotangents), "tm", 1)
    weights = (
        drift_inner,
        drift_hidden.reshape(1, hidden),
        drift_outer,
        drift_offset.reshape(1, width),
        noise_inner,
        noise_hidden.reshape(1, hidden),
        noise_outer,
        noise_offset.reshape(1, width),
    )
    turned = (drift_inner.T, drift_outer.T, noise_inner.T, noise_outer.T)

    def sds(shape, dtype=f32):
        return jax.ShapeDtypeStruct(shape, dtype)

    def forward(incoming, full):
        out_shape = [sds((rows, width))]
        out_specs = [VMEM]
        scratch = [
            pltpu.VMEM((window, rows, width), f32),
            pltpu.SemaphoreType.DMA((window,)),
        ]
        if full:
            out_shape += [
                sds((steps, local_rows, width)),
                sds((steps, rows, width)),
                sds((window, rows, width), bf16),
                sds((window, rows, hidden), bf16),
                sds((window, rows, hidden), bf16),
                sds((window, rows, width)),
            ]
            out_specs += [ANY] * 6
            scratch += [
                pltpu.SemaphoreType.DMA,
                pltpu.VMEM((window, rows, width), f32),
                pltpu.VMEM((window, rows, width), bf16),
                pltpu.VMEM((window, rows, hidden), bf16),
                pltpu.VMEM((window, rows, hidden), bf16),
                pltpu.VMEM((window, rows, width), f32),
            ]
        return pl.pallas_call(
            functools.partial(forward_kernel, full, steps, rows),
            out_shape=out_shape,
            in_specs=[SMEM, VMEM, VMEM, ANY, ANY] + [VMEM] * 8,
            out_specs=out_specs,
            scratch_shapes=scratch,
            compiler_params=PARAMS,
            name="forward_full" if full else "forward_light",
        )(info, initial_state, incoming, increments, mate_noise, *weights)

    incoming = jnp.zeros((rows, width), f32)
    for turn_index in range(stages - 1):
        incoming = moved(forward(incoming, False)[0], 2)
    unused, states, states_send, q, u, v, a = forward(incoming, True)
    states_mate = flipped(states_send, "tm", 1)

    def backward(incoming, full):
        out_shape = [sds((rows, width))]
        out_specs = [VMEM]
        scratch = [
            pltpu.VMEM((window, rows, width), f32),
            pltpu.VMEM((window, rows, hidden), bf16),
            pltpu.VMEM((window, rows, hidden), bf16),
            pltpu.VMEM((window, rows, width), f32),
            pltpu.SemaphoreType.DMA((window,)),
        ]
        if full:
            out_shape += [
                sds((steps, local_rows, width)),
                sds((steps, rows, width)),
                sds((packed_rows, LANES)),
                sds((packed_rows, LANES)),
            ]
            out_specs += [ANY] * 4
            scratch += [
                pltpu.SemaphoreType.DMA,
                pltpu.SemaphoreType.DMA,
                pltpu.VMEM((window, rows, width), bf16),
                pltpu.VMEM((window, rows, width), f32),
                pltpu.VMEM((window, rows, hidden), bf16),
                pltpu.VMEM((window, rows, hidden), bf16),
                pltpu.VMEM((window, rows, width), bf16),
                pltpu.VMEM((window, rows, width), bf16),
                pltpu.VMEM((8, hidden), f32),
                pltpu.VMEM((8, hidden), f32),
                pltpu.VMEM((8, width), f32),
                pltpu.VMEM((8, width), f32),
                pltpu.VMEM((2, packed_rows, LANES), f32),
            ]
        return pl.pallas_call(
            functools.partial(backward_kernel, full, steps, rows, blocks, block_rows),
            out_shape=out_shape,
            in_specs=[SMEM, VMEM] + [ANY] * 6 + [VMEM] * 4,
            out_specs=out_specs,
            scratch_shapes=scratch,
            compiler_params=PARAMS,
            name="backward_full" if full else "backward_light",
        )(info, incoming, cotangents, mate_cotangent, q, u, v, a, *turned)

    incoming = jnp.zeros((rows, width), f32)
    for turn_index in range(stages - 1):
        incoming = moved(backward(incoming, False)[0], -2)
    unused, adjoints, adjoints_send, keep, send = backward(incoming, True)
    mate_grads = flipped(send, "tm", 1)
    adjoints_mate = flipped(adjoints_send, "tm", 1)

    parts = [[keep, mate_grads] for order in orders]
    starts = [[i * color_rows] * 2 for i in range(COLORS)]
    size = color_rows

    def gathered(i, begin, count):
        total = None
        for part, start in zip(parts[i], starts[i]):
            piece = part[start + begin : start + begin + count]
            total = piece if total is None else total + piece
        return total

    for phase in range(len(dims)):
        size //= 2
        arrived = [flipped(gathered(i, 0, size), *orders[i][phase]) for i in range(COLORS)]
        for i in range(COLORS):
            starts[i] = [start + size for start in starts[i]] + [0]
            parts[i].append(arrived[i])
    current = [gathered(i, 0, size) for i in range(COLORS)]
    for phase in reversed(range(1, len(dims))):
        arrived = [flipped(current[i], *orders[i][phase]) for i in range(COLORS)]
        current = [jnp.concatenate([arrived[i], current[i]], 0) for i in range(COLORS)]
    low_mate = [flipped(current[i], "tm", 1) for i in range(COLORS)]
    top = [flipped(current[i], *orders[i][0]) for i in range(COLORS)]
    top_mate = [flipped(top[i], "tm", 1) for i in range(COLORS)]
    pieces = []
    for i in range(COLORS):
        pieces += [current[i], top[i], low_mate[i], top_mate[i]]

    limit = 0.5 * math.sqrt(4 * width * hidden + 2 * hidden + 2 * width)
    shapes = [(width, hidden), (1, hidden), (hidden, width), (1, width)] * 2
    grads = pl.pallas_call(
        functools.partial(finish_kernel, blocks, block_rows, width, hidden, limit),
        out_shape=[sds(shape) for shape in shapes],
        in_specs=[SMEM] + [ANY] * len(pieces),
        out_specs=[VMEM] * 8,
        scratch_shapes=[
            pltpu.VMEM((2, packed_rows, LANES), f32),
            pltpu.SemaphoreType.DMA,
        ],
        compiler_params=PARAMS,
        name="finish",
    )(info, *pieces)
    grads = [g.reshape(-1) if g.shape[0] == 1 else g for g in grads]
    far = (1 - core) * rows
    states = lax.dynamic_update_slice_in_dim(states, states_mate, far, 1)
    adjoints = lax.dynamic_update_slice_in_dim(adjoints, adjoints_mate, far, 1)
    return (states, adjoints, *grads)


def solution(mesh):
    placed = (P("batch", None), P("tm", "batch", None), P("tm", "batch", None)) + (P(),) * 8
    return jax.shard_map(
        shards,
        mesh=mesh,
        in_specs=placed,
        out_specs=(P("tm", "batch", None), P("tm", "batch", None)) + (P(),) * 8,
        check_vma=False,
    )
```

```python
import functools
import math

import jax
import jax.numpy as jnp
from jax import lax
from jax.experimental import pallas as pl
from jax.experimental.pallas import tpu as pltpu
from jax.sharding import PartitionSpec as P

delta_time = 0.05
TILE = 256
LANES = 128
COLORS = 3
PARAMS = pltpu.CompilerParams(vmem_limit_bytes=60 * 1024 * 1024)
ANY = pl.BlockSpec(memory_space=pl.ANY)
VMEM = pl.BlockSpec(memory_space=pltpu.VMEM)
SMEM = pl.BlockSpec(memory_space=pltpu.SMEM)


def accumulators(rows, count):
    return [pltpu.ACC(net)((rows, TILE), jnp.float32) for net in range(2) for i in range(count)]


class Pipe:
    def __init__(self, first, second, accs):
        count = len(accs) // 2
        self.accs = (accs[:count], accs[count:])
        self.tiles = count - 1
        self.first = first
        self.second = second

    def push(self, t):
        t = t % (2 * self.tiles)
        for net in range(2):
            if t < self.tiles:
                tile = self.first[net][:, t * TILE : (t + 1) * TILE]
            else:
                t0 = (t - self.tiles) * TILE
                tile = self.second[net][t0 : t0 + TILE, :]
            pltpu.matmul_push_rhs(tile, staging_register=t % 2, mxu_index=net)

    def prime(self):
        self.push(0)
        self.push(1)

    def run(self, left, act):
        n = self.tiles
        for t in range(n):
            for net in range(2):
                pltpu.matmul_acc_lhs(self.accs[net][t], left[net], load_staged_rhs=t % 2)
            self.push(t + 2)
        for t in range(n, 2 * n):
            hidden = [act(net, t - n, pltpu.matmul_pop(self.accs[net][t - n])) for net in range(2)]
            for net in range(2):
                pltpu.matmul_acc_lhs(self.accs[net][n], hidden[net], load_staged_rhs=t % 2)
            self.push(t + 2)
        return [pltpu.matmul_pop(self.accs[net][n]) for net in range(2)]

    def drain(self, left):
        for net in range(2):
            for t in range(2):
                pltpu.matmul_acc_lhs(self.accs[net][t], left, load_staged_rhs=t)
                pltpu.matmul_pop(self.accs[net][t])


def step_copies(own, received, core, half, rows, steps, buffer, sems, k):
    local = lax.rem(k, steps)
    from_own = pltpu.make_async_copy(
        own.at[local, pl.ds(pl.multiple_of(core * rows, 8), rows), :], buffer.at[k], sems.at[k]
    )
    from_mate = pltpu.make_async_copy(received.at[local], buffer.at[k], sems.at[k])
    return from_own, from_mate


def forward_kernel(
    turn,
    full,
    steps,
    rows,
    info,
    initial,
    own_noise,
    mate_noise,
    drift_inner,
    drift_hidden,
    drift_outer,
    drift_offset,
    noise_inner,
    noise_hidden,
    noise_outer,
    noise_offset,
    *rest,
):
    incoming, rest = (rest[0], rest[1:]) if turn > 0 else (None, rest)
    if full:
        final, states, states_send, q_out, u_out, v_out, a_out = rest[:7]
        noise_buf, in_sems, out_sem, z_buf, q_buf, u_buf, v_buf, a_buf = rest[7:]
    else:
        final, noise_buf, in_sems = rest
    window = 2 * steps
    core = info[0]
    stage = info[1]
    hidden = drift_inner.shape[1]

    def start(k, carry):
        mine = k // steps == core
        from_own, from_mate = step_copies(
            own_noise, mate_noise, core, None, rows, steps, noise_buf, in_sems, k
        )

        @pl.when(mine)
        def _():
            from_own.start()

        @pl.when(jnp.logical_not(mine))
        def _():
            from_mate.start()

        return carry

    def state_copies(k):
        local = lax.rem(k, steps)
        keep = pltpu.make_async_copy(
            z_buf.at[k],
            states.at[local, pl.ds(pl.multiple_of(core * rows, 8), rows), :],
            out_sem,
        )
        send = pltpu.make_async_copy(z_buf.at[k], states_send.at[local], out_sem)
        return keep, send

    def saved_copies(k):
        return [
            pltpu.make_async_copy(buf.at[k], out.at[k], out_sem)
            for buf, out in ((q_buf, q_out), (u_buf, u_out), (v_buf, v_out), (a_buf, a_out))
        ]

    def body(pipe, k, carry):
        pltpu.make_async_copy(mate_noise.at[0], noise_buf.at[k], in_sems.at[k]).wait()
        state = final[...]
        q = state.astype(jnp.bfloat16)
        if full:
            q_buf[k] = q
        saved = (u_buf, v_buf) if full else (None, None)

        def act(net, j, raw):
            cols = slice(j * TILE, (j + 1) * TILE)
            bias = (drift_hidden, noise_hidden)[net]
            value = jnp.tanh(raw + bias[:, cols]).astype(jnp.bfloat16)
            if full:
                saved[net][k, :, cols] = value
            return value

        drift, spread = pipe.run((q, q), act)
        drift = drift + drift_offset[...]
        spread = spread + noise_offset[...]
        s = 0.5 * jnp.tanh(0.5 * spread) + 0.5
        noise = noise_buf[k]
        following = state + delta_time * drift + s * noise
        final[...] = following
        if full:
            a_buf[k] = noise * s * (1.0 - s)
            z_buf[k] = following
            mine = k // steps == core
            keep, send = state_copies(k)

            @pl.when(mine)
            def _():
                keep.start()

            @pl.when(jnp.logical_not(mine))
            def _():
                send.start()

            for copy in saved_copies(k):
                copy.start()
        return carry

    def solve(*accs):
        lax.fori_loop(0, window, start, 0)
        begin = initial[pl.ds(pl.multiple_of(core * rows, 8), rows), :]
        if incoming is not None:
            begin = jnp.where(stage == 0, begin, incoming[...])
        final[...] = begin
        pipe = Pipe((drift_inner, noise_inner), (drift_outer, noise_outer), accs)
        pipe.prime()
        lax.fori_loop(0, window, functools.partial(body, pipe), 0)
        pipe.drain(jnp.zeros((rows, TILE), jnp.bfloat16))

    def guarded(*accs):
        pl.when(stage == turn)(functools.partial(solve, *accs))

    pl.run_scoped(solve if full else guarded, *accumulators(rows, hidden // TILE + 1))
    if full:

        def finish(k, carry):
            state_copies(k)[1].wait()
            for copy in saved_copies(k):
                copy.wait()
            return carry

        lax.fori_loop(0, window, finish, 0)


def backward_kernel(
    turn,
    stages,
    full,
    steps,
    rows,
    blocks,
    block_rows,
    info,
    own_cotangent,
    mate_cotangent,
    q_in,
    u_in,
    v_in,
    a_in,
    drift_inner_t,
    drift_outer_t,
    noise_inner_t,
    noise_outer_t,
    *rest,
):
    incoming, rest = (rest[0], rest[1:]) if turn > 0 else (None, rest)
    if full:
        final, adjoints, adjoints_send, keep_out, send_out = rest[:5]
        (c_buf, u_buf, v_buf, a_buf, in_sems, q_sem, out_sem, q_buf) = rest[5:13]
        (e_buf, pb_buf, rb_buf, fb_buf, gb_buf, qt_buf) = rest[13:19]
        (p_sum, r_sum, f_sum, g_sum, packed) = rest[19:]
    else:
        final, c_buf, u_buf, v_buf, a_buf, in_sems = rest
    window = 2 * steps
    core = info[0]
    stage = info[1]
    width, hidden = drift_outer_t.shape

    def saved_copies(k):
        return [
            pltpu.make_async_copy(src.at[k], buf.at[k], in_sems.at[k])
            for src, buf in ((u_in, u_buf), (v_in, v_buf), (a_in, a_buf))
        ]

    def start(n, carry):
        k = window - 1 - n
        mine = k // steps == core
        from_own, from_mate = step_copies(
            own_cotangent, mate_cotangent, core, None, rows, steps, c_buf, in_sems, k
        )

        @pl.when(mine)
        def _():
            from_own.start()

        @pl.when(jnp.logical_not(mine))
        def _():
            from_mate.start()

        for copy in saved_copies(k):
            copy.start()
        return carry

    def adjoint_copies(k):
        local = lax.rem(k, steps)
        keep = pltpu.make_async_copy(
            e_buf.at[k],
            adjoints.at[local, pl.ds(pl.multiple_of(core * rows, 8), rows), :],
            out_sem,
        )
        send = pltpu.make_async_copy(e_buf.at[k], adjoints_send.at[local], out_sem)
        return keep, send

    def partial(x):
        return jnp.sum(x.reshape(rows // 8, 8, x.shape[1]), 0)

    def body(pipe, n, carry):
        k = window - 1 - n
        pltpu.make_async_copy(mate_cotangent.at[0], c_buf.at[k], in_sems.at[k]).wait()
        for copy in saved_copies(k):
            copy.wait()
        w = final[...] + c_buf[k]
        final[...] = w
        f = delta_time * w
        g = w * a_buf[k]
        fb = f.astype(jnp.bfloat16)
        gb = g.astype(jnp.bfloat16)
        if full:
            fb_buf[:, pl.ds(pl.multiple_of(k * rows, rows), rows)] = fb.T
            gb_buf[:, pl.ds(pl.multiple_of(k * rows, rows), rows)] = gb.T
            qt_buf[:, pl.ds(pl.multiple_of(k * rows, rows), rows)] = q_buf[k].T
            f_sum[...] += partial(f)
            g_sum[...] += partial(g)

        def act(net, j, raw):
            cols = slice(j * TILE, (j + 1) * TILE)
            value = (u_buf, v_buf)[net][k, :, cols].astype(jnp.float32)
            back = raw * (1.0 - value * value)
            low = back.astype(jnp.bfloat16)
            if full:
                (p_sum, r_sum)[net][:, cols] += partial(back)
                (pb_buf, rb_buf)[net][k, :, cols] = low
            return low

        drift_part, noise_part = pipe.run((fb, gb), act)
        result = final[...] + (drift_part + noise_part)
        final[...] = result
        if full:
            e_buf[k] = result
            mine = k // steps == core
            keep, send = adjoint_copies(k)

            @pl.when(mine)
            def _():
                keep.start()

            @pl.when(jnp.logical_not(mine))
            def _():
                send.start()

        return carry

    def solve(*accs):
        lax.fori_loop(0, window, start, 0)
        if full:
            q_copy = pltpu.make_async_copy(q_in, q_buf, q_sem)
            q_copy.start()
            for ref in (p_sum, r_sum, f_sum, g_sum):
                ref[...] = jnp.zeros_like(ref)
            q_copy.wait()
        begin = jnp.zeros(final.shape, jnp.float32)
        if incoming is not None:
            begin = jnp.where(stage == stages - 1, begin, incoming[...])
        final[...] = begin
        pipe = Pipe((drift_outer_t, noise_outer_t), (drift_inner_t, noise_inner_t), accs)
        pipe.prime()
        lax.fori_loop(0, window, functools.partial(body, pipe), 0)
        pipe.drain(jnp.zeros((rows, TILE), jnp.bfloat16))

    def guarded(*accs):
        pl.when(stage == stages - 1 - turn)(functools.partial(solve, *accs))

    pl.run_scoped(solve if full else guarded, *accumulators(rows, hidden // TILE + 1))
    if not full:
        return
    total = window * rows
    per_matrix = width * hidden // LANES
    lefts = ((qt_buf, fb_buf), (qt_buf, gb_buf))
    rights = ((pb_buf, u_buf), (rb_buf, v_buf))

    def products(*accs):
        per_step = TILE // rows
        chain = [
            (j, which, c)
            for j in range(hidden // TILE)
            for which in range(2)
            for c in range(total // TILE)
        ]

        def push(n):
            j, which, c = chain[n]
            for net in range(2):
                block = rights[net][which][
                    c * per_step : (c + 1) * per_step, :, j * TILE : (j + 1) * TILE
                ]
                pltpu.matmul_push_rhs(
                    block.reshape(TILE, TILE), staging_register=n % 2, mxu_index=net
                )

        push(0)
        push(1)
        for n, (j, which, c) in enumerate(chain):
            slot = (2 * j + which) % 4
            for net in range(2):
                left = lefts[net][which][:, c * TILE : (c + 1) * TILE]
                pltpu.matmul_acc_lhs(accs[4 * net + slot], left, load_staged_rhs=n % 2)
            if n + 2 < len(chain):
                push(n + 2)
            if c == total // TILE - 1:
                for net in range(2):
                    grad = pltpu.matmul_pop(accs[4 * net + slot])
                    for i in range(TILE // LANES):
                        row = which * per_matrix + (j * (TILE // LANES) + i) * width
                        packed[net, row : row + width, :] = grad[:, i * LANES : (i + 1) * LANES]

    pl.run_scoped(products, *accumulators(width, 4))
    for net, (hidden_sum, offset_sum) in enumerate(((p_sum, f_sum), (r_sum, g_sum))):
        base = 2 * per_matrix
        hidden_total = jnp.sum(hidden_sum[...], 0, keepdims=True)
        offset_total = jnp.sum(offset_sum[...], 0, keepdims=True)
        packed[net, base:, :] = jnp.zeros((packed.shape[1] - base, LANES), jnp.float32)
        for i in range(hidden // LANES):
            packed[net, base + i : base + i + 1, :] = hidden_total[:, i * LANES : (i + 1) * LANES]
        base += hidden // LANES
        for i in range(width // LANES):
            packed[net, base + i : base + i + 1, :] = offset_total[:, i * LANES : (i + 1) * LANES]

    def grad_copies(out, net):
        copies = []
        for color in range(COLORS):
            me = info[2 + color]
            for s in range(blocks):
                source = (color * blocks + s) * block_rows
                place = color * blocks + ((s ^ (blocks - 1)) ^ me)
                copies.append(
                    pltpu.make_async_copy(
                        packed.at[net, pl.ds(source, block_rows), :],
                        out.at[pl.ds(pl.multiple_of(place * block_rows, 8), block_rows), :],
                        out_sem,
                    )
                )
        return copies

    for copy in grad_copies(send_out, 1 - core) + grad_copies(keep_out, core):
        copy.start()

    def finish(k, carry):
        adjoint_copies(k)[1].wait()
        return carry

    lax.fori_loop(0, window, finish, 0)
    for copy in grad_copies(send_out, 1 - core) + grad_copies(keep_out, core):
        copy.wait()


def finish_kernel(blocks, block_rows, width, hidden, limit, info, *rest):
    pieces = rest[: 4 * COLORS]
    outs = rest[4 * COLORS : 4 * COLORS + 8]
    packed, sem = rest[4 * COLORS + 8 :]
    core = info[0]
    half = blocks // 2
    copies = []
    for color in range(COLORS):
        me = info[2 + color]
        for side in range(2):
            net = core if side == 0 else 1 - core
            for top in range(2):
                piece = pieces[color * 4 + side * 2 + top]
                for p in range(half):
                    s = (top * half + half - 1 - p) ^ me
                    place = (color * blocks + s) * block_rows
                    copies.append(
                        pltpu.make_async_copy(
                            piece.at[pl.ds(p * block_rows, block_rows), :],
                            packed.at[net, pl.ds(pl.multiple_of(place, 8), block_rows), :],
                            sem,
                        )
                    )
    for copy in copies:
        copy.start()
    for copy in copies:
        copy.wait()
    chunk = block_rows * blocks * COLORS // 8
    acc = jnp.zeros((8, LANES), jnp.float32)
    for net in range(2):
        whole = packed[net]
        acc = acc + jnp.sum(jnp.square(whole).reshape(chunk, 8, LANES), 0)
    total = jnp.sum(jnp.sum(acc, 1, keepdims=True), 0, keepdims=True)
    factor = jnp.minimum(1.0, limit / jnp.sqrt(total))
    per_matrix = width * hidden // LANES
    for net in range(2):
        inner, hidden_out, outer, offset_out = outs[net * 4 : net * 4 + 4]
        for j in range(hidden // LANES):
            lanes = slice(j * LANES, (j + 1) * LANES)
            inner[:, lanes] = packed[net, j * width : (j + 1) * width, :] * factor
            row = per_matrix + j * width
            outer[lanes, :] = (packed[net, row : row + width, :] * factor).T
        base = 2 * per_matrix
        for j in range(hidden // LANES):
            hidden_out[:, j * LANES : (j + 1) * LANES] = packed[net, base + j : base + j + 1, :] * factor
        base += hidden // LANES
        for j in range(width // LANES):
            offset_out[:, j * LANES : (j + 1) * LANES] = packed[net, base + j : base + j + 1, :] * factor


def flipped(block, axis, bit):
    return lax.ppermute(block, axis, [(i, i ^ bit) for i in range(lax.axis_size(axis))])


def moved(block, distance):
    count = lax.axis_size("tm")
    return lax.ppermute(
        block, "tm", [(i, i + distance) for i in range(count) if 0 <= i + distance < count]
    )


def bits_of(size):
    return [1 << i for i in range(size.bit_length() - 1)]


def shards(
    initial_state,
    increments,
    cotangents,
    drift_inner,
    drift_hidden,
    drift_outer,
    drift_offset,
    noise_inner,
    noise_hidden,
    noise_outer,
    noise_offset,
):
    f32, bf16 = jnp.float32, jnp.bfloat16
    segments = lax.axis_size("tm")
    segment = lax.axis_index("tm")
    group = lax.axis_index("batch")
    core = segment % 2
    stages = segments // 2
    stage = segment // 2
    steps, local_rows, width = increments.shape
    hidden = drift_inner.shape[1]
    rows = local_rows // 2
    window = 2 * steps

    dims = [("tm", bit) for bit in bits_of(segments)[1:]]
    dims += [("batch", bit) for bit in bits_of(lax.axis_size("batch"))]
    turn = min(COLORS, len(dims))
    orders = [dims[i % turn : turn] + dims[: i % turn] + dims[turn:] for i in range(COLORS)]
    blocks = 1 << len(dims)
    used = (2 * width * hidden + hidden + width) // LANES
    block_rows = 8 * (-(-used // (8 * blocks * COLORS)))
    color_rows = blocks * block_rows
    packed_rows = COLORS * color_rows

    def position(order):
        place = jnp.int32(0)
        for axis, bit in order:
            index = segment if axis == "tm" else group
            place = 2 * place + (index // bit) % 2
        return place

    info = jnp.stack([core, stage] + [position(order) for order in orders]).astype(jnp.int32)

    def other_half(array):
        return lax.dynamic_slice_in_dim(array, (1 - core) * rows, rows, 1)

    mate_noise = flipped(other_half(increments), "tm", 1)
    mate_cotangent = flipped(other_half(cotangents), "tm", 1)
    weights = (
        drift_inner,
        drift_hidden.reshape(1, hidden),
        drift_outer,
        drift_offset.reshape(1, width),
        noise_inner,
        noise_hidden.reshape(1, hidden),
        noise_outer,
        noise_offset.reshape(1, width),
    )
    turned = (drift_inner.T, drift_outer.T, noise_inner.T, noise_outer.T)

    def sds(shape, dtype=f32):
        return jax.ShapeDtypeStruct(shape, dtype)

    def forward(incoming, turn, full):
        out_shape = [sds((rows, width))]
        out_specs = [VMEM]
        scratch = [
            pltpu.VMEM((window, rows, width), f32),
            pltpu.SemaphoreType.DMA((window,)),
        ]
        if full:
            out_shape += [
                sds((steps, local_rows, width)),
                sds((steps, rows, width)),
                sds((window, rows, width), bf16),
                sds((window, rows, hidden), bf16),
                sds((window, rows, hidden), bf16),
                sds((window, rows, width)),
            ]
            out_specs += [ANY] * 6
            scratch += [
                pltpu.SemaphoreType.DMA,
                pltpu.VMEM((window, rows, width), f32),
                pltpu.VMEM((window, rows, width), bf16),
                pltpu.VMEM((window, rows, hidden), bf16),
                pltpu.VMEM((window, rows, hidden), bf16),
                pltpu.VMEM((window, rows, width), f32),
            ]
        return pl.pallas_call(
            functools.partial(forward_kernel, turn, full, steps, rows),
            out_shape=out_shape,
            in_specs=[SMEM, VMEM, ANY, ANY] + [VMEM] * (8 + (turn > 0)),
            out_specs=out_specs,
            scratch_shapes=scratch,
            compiler_params=PARAMS,
            name="forward_full" if full else "forward_light",
        )(info, initial_state, increments, mate_noise, *weights, *incoming)

    def relay(run, distance, reached):
        incoming = ()
        for turn in range(stages - 1):
            arrived = moved(run(incoming, turn, False)[0], distance)
            if turn > 0:
                arrived = jnp.where(reached == turn + 1, arrived, incoming[0])
            incoming = (arrived,)
        return run(incoming, stages - 1, True)

    unused, states, states_send, q, u, v, a = relay(forward, 2, stage)
    states_mate = flipped(states_send, "tm", 1)

    def backward(incoming, turn, full):
        out_shape = [sds((rows, width))]
        out_specs = [VMEM]
        scratch = [
            pltpu.VMEM((window, rows, width), f32),
            pltpu.VMEM((window, rows, hidden), bf16),
            pltpu.VMEM((window, rows, hidden), bf16),
            pltpu.VMEM((window, rows, width), f32),
            pltpu.SemaphoreType.DMA((window,)),
        ]
        if full:
            out_shape += [
                sds((steps, local_rows, width)),
                sds((steps, rows, width)),
                sds((packed_rows, LANES)),
                sds((packed_rows, LANES)),
            ]
            out_specs += [ANY] * 4
            scratch += [
                pltpu.SemaphoreType.DMA,
                pltpu.SemaphoreType.DMA,
                pltpu.VMEM((window, rows, width), bf16),
                pltpu.VMEM((window, rows, width), f32),
                pltpu.VMEM((window, rows, hidden), bf16),
                pltpu.VMEM((window, rows, hidden), bf16),
                pltpu.VMEM((width, window * rows), bf16),
                pltpu.VMEM((width, window * rows), bf16),
                pltpu.VMEM((width, window * rows), bf16),
                pltpu.VMEM((8, hidden), f32),
                pltpu.VMEM((8, hidden), f32),
                pltpu.VMEM((8, width), f32),
                pltpu.VMEM((8, width), f32),
                pltpu.VMEM((2, packed_rows, LANES), f32),
            ]
        return pl.pallas_call(
            functools.partial(
                backward_kernel, turn, stages, full, steps, rows, blocks, block_rows
            ),
            out_shape=out_shape,
            in_specs=[SMEM] + [ANY] * 6 + [VMEM] * (4 + (turn > 0)),
            out_specs=out_specs,
            scratch_shapes=scratch,
            compiler_params=PARAMS,
            name="backward_full" if full else "backward_light",
        )(info, cotangents, mate_cotangent, q, u, v, a, *turned, *incoming)

    unused, adjoints, adjoints_send, keep, send = relay(backward, -2, stages - 1 - stage)
    mate_grads = flipped(send, "tm", 1)
    adjoints_mate = flipped(adjoints_send, "tm", 1)

    parts = [[keep, mate_grads] for order in orders]
    starts = [[i * color_rows] * 2 for i in range(COLORS)]
    size = color_rows

    def gathered(i, begin, count):
        total = None
        for part, start in zip(parts[i], starts[i]):
            piece = part[start + begin : start + begin + count]
            total = piece if total is None else total + piece
        return total

    for phase in range(len(dims)):
        size //= 2
        arrived = [flipped(gathered(i, 0, size), *orders[i][phase]) for i in range(COLORS)]
        for i in range(COLORS):
            starts[i] = [start + size for start in starts[i]] + [0]
            parts[i].append(arrived[i])
    current = [gathered(i, 0, size) for i in range(COLORS)]
    for phase in reversed(range(1, len(dims))):
        arrived = [flipped(current[i], *orders[i][phase]) for i in range(COLORS)]
        current = [jnp.concatenate([arrived[i], current[i]], 0) for i in range(COLORS)]
    low_mate = [flipped(current[i], "tm", 1) for i in range(COLORS)]
    top = [flipped(current[i], *orders[i][0]) for i in range(COLORS)]
    top_mate = [flipped(top[i], "tm", 1) for i in range(COLORS)]
    pieces = []
    for i in range(COLORS):
        pieces += [current[i], top[i], low_mate[i], top_mate[i]]

    limit = 0.5 * math.sqrt(4 * width * hidden + 2 * hidden + 2 * width)
    shapes = [(width, hidden), (1, hidden), (hidden, width), (1, width)] * 2
    grads = pl.pallas_call(
        functools.partial(finish_kernel, blocks, block_rows, width, hidden, limit),
        out_shape=[sds(shape) for shape in shapes],
        in_specs=[SMEM] + [ANY] * len(pieces),
        out_specs=[VMEM] * 8,
        scratch_shapes=[
            pltpu.VMEM((2, packed_rows, LANES), f32),
            pltpu.SemaphoreType.DMA,
        ],
        compiler_params=PARAMS,
        name="finish",
    )(info, *pieces)
    grads = [g.reshape(-1) if g.shape[0] == 1 else g for g in grads]
    far = (1 - core) * rows
    states = lax.dynamic_update_slice_in_dim(states, states_mate, far, 1)
    adjoints = lax.dynamic_update_slice_in_dim(adjoints, adjoints_mate, far, 1)
    return (states, adjoints, *grads)


def solution(mesh):
    placed = (P("batch", None), P("tm", "batch", None), P("tm", "batch", None)) + (P(),) * 8
    return jax.shard_map(
        shards,
        mesh=mesh,
        in_specs=placed,
        out_specs=(P("tm", "batch", None), P("tm", "batch", None)) + (P(),) * 8,
        check_vma=False,
    )
```

```python
import functools
import math

import jax
import jax.numpy as jnp
from jax import lax
from jax.experimental import pallas as pl
from jax.experimental.pallas import tpu as pltpu
from jax.sharding import PartitionSpec as P

delta_time = 0.05
TILE = 256
LANES = 128
COLORS = 3
AHEAD = 4
PARAMS = pltpu.CompilerParams(vmem_limit_bytes=60 * 1024 * 1024)
ANY = pl.BlockSpec(memory_space=pl.ANY)
VMEM = pl.BlockSpec(memory_space=pltpu.VMEM)
SMEM = pl.BlockSpec(memory_space=pltpu.SMEM)


def accumulators(rows, count):
    return [pltpu.ACC(net)((rows, TILE), jnp.float32) for net in range(2) for i in range(count)]


class Pipe:
    def __init__(self, first, second, accs):
        count = len(accs) // 2
        self.accs = (accs[:count], accs[count:])
        self.tiles = count - 1
        self.first = first
        self.second = second

    def push(self, t):
        t = t % (2 * self.tiles)
        for net in range(2):
            if t < self.tiles:
                tile = self.first[net][t]
            else:
                t0 = (t - self.tiles) * TILE
                tile = self.second[net][t0 : t0 + TILE, :]
            pltpu.matmul_push_rhs(tile, staging_register=t % 2, mxu_index=net)

    def prime(self):
        self.push(0)
        self.push(1)

    def run(self, left, act):
        n = self.tiles
        for t in range(n):
            for net in range(2):
                pltpu.matmul_acc_lhs(self.accs[net][t], left[net], load_staged_rhs=t % 2)
            self.push(t + 2)
        for t in range(n, 2 * n):
            hidden = [act(net, t - n, pltpu.matmul_pop(self.accs[net][t - n])) for net in range(2)]
            for net in range(2):
                pltpu.matmul_acc_lhs(self.accs[net][n], hidden[net], load_staged_rhs=t % 2)
            self.push(t + 2)
        return [pltpu.matmul_pop(self.accs[net][n]) for net in range(2)]

    def drain(self, left):
        for net in range(2):
            for t in range(2):
                pltpu.matmul_acc_lhs(self.accs[net][t], left, load_staged_rhs=t)
                pltpu.matmul_pop(self.accs[net][t])


def start_step(own, received, core, rows, steps, buffer, sems, k):
    local = lax.rem(k, steps)
    mine = k // steps == core

    @pl.when(mine)
    def _():
        source = own.at[local, pl.ds(pl.multiple_of(core * rows, 8), rows), :]
        pltpu.make_async_copy(source, buffer.at[k], sems.at[k]).start()

    @pl.when(jnp.logical_not(mine))
    def _():
        pltpu.make_async_copy(received.at[local], buffer.at[k], sems.at[k]).start()


def store_step(source, kept, sent, core, rows, steps, sem, k):
    local = lax.rem(k, steps)
    mine = k // steps == core

    @pl.when(mine)
    def _():
        target = kept.at[local, pl.ds(pl.multiple_of(core * rows, 8), rows), :]
        pltpu.make_async_copy(source, target, sem).start()

    @pl.when(jnp.logical_not(mine))
    def _():
        pltpu.make_async_copy(source, sent.at[local], sem).start()


def weight_copies(first, second, first_buf, second_buf, sem):
    copies = []
    for net in range(2):
        for j in range(first_buf.shape[1]):
            tile = first[net].at[:, pl.ds(j * TILE, TILE)]
            copies.append(pltpu.make_async_copy(tile, first_buf.at[net, j], sem))
    for net in range(2):
        copies.append(pltpu.make_async_copy(second[net], second_buf.at[net], sem))
    return copies


def forward_kernel(
    turn,
    full,
    steps,
    rows,
    info,
    initial,
    own_noise,
    mate_noise,
    drift_inner,
    drift_hidden,
    drift_outer,
    drift_offset,
    noise_inner,
    noise_hidden,
    noise_outer,
    noise_offset,
    *rest,
):
    incoming, rest = (rest[0], rest[1:]) if turn > 0 else (None, rest)
    if full:
        final, states, states_send, q_out, u_out, v_out, a_out = rest[:7]
        noise_buf, in_sems, weight_sem, first_buf, second_buf = rest[7:12]
        out_sem, z_buf, q_buf, u_buf, v_buf, a_buf = rest[12:]
    else:
        final, noise_buf, in_sems, weight_sem, first_buf, second_buf = rest
    window = 2 * steps
    core = info[0]
    stage = info[1]
    hidden = drift_inner.shape[1]
    weights = weight_copies(
        (drift_inner, noise_inner), (drift_outer, noise_outer), first_buf, second_buf, weight_sem
    )
    if incoming is None:
        begin = initial.at[pl.ds(pl.multiple_of(core * rows, 8), rows), :]
        weights.append(pltpu.make_async_copy(begin, final, weight_sem))

    def fetch(k):
        start_step(own_noise, mate_noise, core, rows, steps, noise_buf, in_sems, k)

    def saved_copies(k):
        return [
            pltpu.make_async_copy(buf.at[k], out.at[k], out_sem)
            for buf, out in ((q_buf, q_out), (a_buf, a_out))
        ] + [
            pltpu.make_async_copy(buf.at[:, k], out.at[:, k], out_sem)
            for buf, out in ((u_buf, u_out), (v_buf, v_out))
        ]

    def body(pipe, k, carry):
        pltpu.make_async_copy(mate_noise.at[0], noise_buf.at[k], in_sems.at[k]).wait()
        state = final[...]
        q = state.astype(jnp.bfloat16)
        if full:
            q_buf[k] = q
        saved = (u_buf, v_buf) if full else (None, None)

        def act(net, j, raw):
            cols = slice(j * TILE, (j + 1) * TILE)
            bias = (drift_hidden, noise_hidden)[net]
            value = jnp.tanh(raw + bias[:, cols]).astype(jnp.bfloat16)
            if full:
                saved[net][j, k] = value
            return value

        @pl.when(k + AHEAD < window)
        def _():
            fetch(k + AHEAD)

        drift, spread = pipe.run((q, q), act)
        drift = drift + drift_offset[...]
        spread = spread + noise_offset[...]
        s = 0.5 * jnp.tanh(0.5 * spread) + 0.5
        noise = noise_buf[k]
        following = state + delta_time * drift + s * noise
        final[...] = following
        if full:
            a_buf[k] = noise * s * (1.0 - s)
            z_buf[k] = following
            store_step(z_buf.at[k], states, states_send, core, rows, steps, out_sem, k)
            for copy in saved_copies(k):
                copy.start()
        return carry

    def solve(*accs):
        for copy in weights:
            copy.start()
        for k in range(AHEAD):
            fetch(k)
        for copy in weights:
            copy.wait()
        if incoming is not None:
            begin = initial[pl.ds(pl.multiple_of(core * rows, 8), rows), :]
            final[...] = jnp.where(stage == 0, begin, incoming[...])
        pipe = Pipe(
            [first_buf.at[net] for net in range(2)], [second_buf.at[net] for net in range(2)], accs
        )
        pipe.prime()
        lax.fori_loop(0, window, functools.partial(body, pipe), 0)
        pipe.drain(jnp.zeros((rows, TILE), jnp.bfloat16))

    def guarded(*accs):
        pl.when(stage == turn)(functools.partial(solve, *accs))

    pl.run_scoped(solve if full else guarded, *accumulators(rows, hidden // TILE + 1))
    if full:

        def finish(k, carry):
            pltpu.make_async_copy(z_buf.at[k], states_send.at[0], out_sem).wait()
            for copy in saved_copies(k):
                copy.wait()
            return carry

        lax.fori_loop(0, window, finish, 0)


def backward_kernel(
    turn,
    stages,
    full,
    steps,
    rows,
    blocks,
    block_rows,
    info,
    own_cotangent,
    mate_cotangent,
    q_in,
    u_in,
    v_in,
    a_in,
    drift_inner_t,
    drift_outer_t,
    noise_inner_t,
    noise_outer_t,
    *rest,
):
    incoming, rest = (rest[0], rest[1:]) if turn > 0 else (None, rest)
    if full:
        final, adjoints, adjoints_send, keep_out, send_out = rest[:5]
        rest = rest[5:]
    else:
        final, rest = rest[0], rest[1:]
    c_buf, u_buf, v_buf, a_buf, in_sems, weight_sem, first_buf, second_buf = rest[:8]
    if full:
        (out_sem, q_buf, e_buf, pb_buf, rb_buf, fb_buf, gb_buf, qt_buf) = rest[8:16]
        (p_sum, r_sum, f_sum, g_sum, packed) = rest[16:]
    window = 2 * steps
    core = info[0]
    stage = info[1]
    width, hidden = drift_outer_t.shape
    weights = weight_copies(
        (drift_outer_t, noise_outer_t),
        (drift_inner_t, noise_inner_t),
        first_buf,
        second_buf,
        weight_sem,
    )

    def saved_copies(k):
        whole = ((a_in, a_buf), (q_in, q_buf)) if full else ((a_in, a_buf),)
        return [pltpu.make_async_copy(src.at[k], buf.at[k], in_sems.at[k]) for src, buf in whole] + [
            pltpu.make_async_copy(src.at[:, k], buf.at[:, k], in_sems.at[k])
            for src, buf in ((u_in, u_buf), (v_in, v_buf))
        ]

    def fetch(k):
        start_step(own_cotangent, mate_cotangent, core, rows, steps, c_buf, in_sems, k)
        for copy in saved_copies(k):
            copy.start()

    def partial(x):
        return jnp.sum(x.reshape(rows // 8, 8, x.shape[1]), 0)

    def body(pipe, n, carry):
        k = window - 1 - n
        pltpu.make_async_copy(mate_cotangent.at[0], c_buf.at[k], in_sems.at[k]).wait()
        for copy in saved_copies(k):
            copy.wait()
        w = final[...] + c_buf[k]
        final[...] = w
        f = delta_time * w
        g = w * a_buf[k]
        fb = f.astype(jnp.bfloat16)
        gb = g.astype(jnp.bfloat16)
        if full:
            part = k // per_tile
            lanes = pl.ds(pl.multiple_of(lax.rem(k, per_tile) * rows, rows), rows)
            fb_buf[part, :, lanes] = fb.T
            gb_buf[part, :, lanes] = gb.T
            qt_buf[part, :, lanes] = q_buf[k].T
            f_sum[...] += partial(f)
            g_sum[...] += partial(g)

        def act(net, j, raw):
            cols = slice(j * TILE, (j + 1) * TILE)
            value = (u_buf, v_buf)[net][j, k].astype(jnp.float32)
            back = raw * (1.0 - value * value)
            low = back.astype(jnp.bfloat16)
            if full:
                (p_sum, r_sum)[net][:, cols] += partial(back)
                (pb_buf, rb_buf)[net][j, k] = low
            return low

        @pl.when(k >= AHEAD)
        def _():
            fetch(k - AHEAD)

        drift_part, noise_part = pipe.run((fb, gb), act)
        result = final[...] + (drift_part + noise_part)
        final[...] = result
        if full:
            e_buf[k] = result
            store_step(e_buf.at[k], adjoints, adjoints_send, core, rows, steps, out_sem, k)
        return carry

    per_tile = TILE // rows

    def solve(*accs):
        for copy in weights:
            copy.start()
        for n in range(AHEAD):
            fetch(window - 1 - n)
        if full:
            for ref in (p_sum, r_sum, f_sum, g_sum):
                ref[...] = jnp.zeros_like(ref)
        begin = jnp.zeros(final.shape, jnp.float32)
        if incoming is not None:
            begin = jnp.where(stage == stages - 1, begin, incoming[...])
        final[...] = begin
        for copy in weights:
            copy.wait()
        pipe = Pipe(
            [first_buf.at[net] for net in range(2)], [second_buf.at[net] for net in range(2)], accs
        )
        pipe.prime()
        lax.fori_loop(0, window, functools.partial(body, pipe), 0)
        pipe.drain(jnp.zeros((rows, TILE), jnp.bfloat16))

    def guarded(*accs):
        pl.when(stage == stages - 1 - turn)(functools.partial(solve, *accs))

    pl.run_scoped(solve if full else guarded, *accumulators(rows, hidden // TILE + 1))
    if not full:
        return
    total = window * rows
    per_matrix = width * hidden // LANES
    lefts = ((qt_buf, fb_buf), (qt_buf, gb_buf))
    rights = ((pb_buf, u_buf), (rb_buf, v_buf))

    def products(*accs):
        chain = [
            (j, which, c)
            for j in range(hidden // TILE)
            for which in range(2)
            for c in range(total // TILE)
        ]

        def push(n):
            j, which, c = chain[n]
            for net in range(2):
                block = rights[net][which][j, c * per_tile : (c + 1) * per_tile]
                pltpu.matmul_push_rhs(
                    block.reshape(TILE, TILE), staging_register=n % 2, mxu_index=net
                )

        push(0)
        push(1)
        for n, (j, which, c) in enumerate(chain):
            slot = (2 * j + which) % 4
            for net in range(2):
                left = lefts[net][which][c]
                pltpu.matmul_acc_lhs(accs[4 * net + slot], left, load_staged_rhs=n % 2)
            if n + 2 < len(chain):
                push(n + 2)
            if c == total // TILE - 1:
                for net in range(2):
                    grad = pltpu.matmul_pop(accs[4 * net + slot])
                    for i in range(TILE // LANES):
                        row = which * per_matrix + (j * (TILE // LANES) + i) * width
                        packed[net, row : row + width, :] = grad[:, i * LANES : (i + 1) * LANES]
                        done[row // width] = True
                release()

    for net, (hidden_sum, offset_sum) in enumerate(((p_sum, f_sum), (r_sum, g_sum))):
        base = 2 * per_matrix
        hidden_total = jnp.sum(hidden_sum[...], 0, keepdims=True)
        offset_total = jnp.sum(offset_sum[...], 0, keepdims=True)
        packed[net, base:, :] = jnp.zeros((packed.shape[1] - base, LANES), jnp.float32)
        for i in range(hidden // LANES):
            packed[net, base + i : base + i + 1, :] = hidden_total[:, i * LANES : (i + 1) * LANES]
        base += hidden // LANES
        for i in range(width // LANES):
            packed[net, base + i : base + i + 1, :] = offset_total[:, i * LANES : (i + 1) * LANES]

    every_block = [(color, b) for color in range(COLORS) for b in range(blocks)]

    def grad_copies(color, b):
        source = (color * blocks + b) * block_rows
        place = color * blocks + ((b ^ (blocks - 1)) ^ info[2 + color])
        target = pl.ds(pl.multiple_of(place * block_rows, 8), block_rows)
        return [
            pltpu.make_async_copy(
                packed.at[net, pl.ds(source, block_rows), :], out.at[target, :], out_sem
            )
            for out, net in ((send_out, 1 - core), (keep_out, core))
        ]

    waiting = list(every_block)
    done = [False] * (2 * per_matrix // width)

    def release():
        for color, b in list(waiting):
            begin = (color * blocks + b) * block_rows
            end = min(begin + block_rows, 2 * per_matrix)
            if all(done[row // width] for row in range(begin, end)):
                waiting.remove((color, b))
                for copy in grad_copies(color, b):
                    copy.start()

    pl.run_scoped(products, *accumulators(width, 4))

    def finish(k, carry):
        pltpu.make_async_copy(e_buf.at[k], adjoints_send.at[0], out_sem).wait()
        return carry

    lax.fori_loop(0, window, finish, 0)
    for color, b in every_block:
        for copy in grad_copies(color, b):
            copy.wait()


def finish_kernel(blocks, block_rows, width, hidden, limit, info, *rest):
    pieces = rest[: 4 * COLORS]
    outs = rest[4 * COLORS : 4 * COLORS + 8]
    packed, sem = rest[4 * COLORS + 8 :]
    core = info[0]
    half = blocks // 2
    copies = []
    for color in range(COLORS):
        me = info[2 + color]
        for side in range(2):
            net = core if side == 0 else 1 - core
            for top in range(2):
                piece = pieces[color * 4 + side * 2 + top]
                for p in range(half):
                    s = (top * half + half - 1 - p) ^ me
                    place = (color * blocks + s) * block_rows
                    copies.append(
                        pltpu.make_async_copy(
                            piece.at[pl.ds(p * block_rows, block_rows), :],
                            packed.at[net, pl.ds(pl.multiple_of(place, 8), block_rows), :],
                            sem,
                        )
                    )
    for copy in copies:
        copy.start()
    for copy in copies:
        copy.wait()
    chunk = block_rows * blocks * COLORS // 8
    acc = jnp.zeros((8, LANES), jnp.float32)
    for net in range(2):
        whole = packed[net]
        acc = acc + jnp.sum(jnp.square(whole).reshape(chunk, 8, LANES), 0)
    total = jnp.sum(jnp.sum(acc, 1, keepdims=True), 0, keepdims=True)
    factor = jnp.minimum(1.0, limit / jnp.sqrt(total))
    per_matrix = width * hidden // LANES
    for net in range(2):
        inner, hidden_out, outer, offset_out = outs[net * 4 : net * 4 + 4]
        for j in range(hidden // LANES):
            lanes = slice(j * LANES, (j + 1) * LANES)
            inner[:, lanes] = packed[net, j * width : (j + 1) * width, :] * factor
            row = per_matrix + j * width
            outer[lanes, :] = (packed[net, row : row + width, :] * factor).T
        base = 2 * per_matrix
        for j in range(hidden // LANES):
            hidden_out[:, j * LANES : (j + 1) * LANES] = packed[net, base + j : base + j + 1, :] * factor
        base += hidden // LANES
        for j in range(width // LANES):
            offset_out[:, j * LANES : (j + 1) * LANES] = packed[net, base + j : base + j + 1, :] * factor


def flipped(block, axis, bit):
    return lax.ppermute(block, axis, [(i, i ^ bit) for i in range(lax.axis_size(axis))])


def moved(block, distance):
    count = lax.axis_size("tm")
    return lax.ppermute(
        block, "tm", [(i, i + distance) for i in range(count) if 0 <= i + distance < count]
    )


def bits_of(size):
    return [1 << i for i in range(size.bit_length() - 1)]


def shards(
    initial_state,
    increments,
    cotangents,
    drift_inner,
    drift_hidden,
    drift_outer,
    drift_offset,
    noise_inner,
    noise_hidden,
    noise_outer,
    noise_offset,
):
    f32, bf16 = jnp.float32, jnp.bfloat16
    segments = lax.axis_size("tm")
    segment = lax.axis_index("tm")
    group = lax.axis_index("batch")
    core = segment % 2
    stages = segments // 2
    stage = segment // 2
    steps, local_rows, width = increments.shape
    hidden = drift_inner.shape[1]
    rows = local_rows // 2
    window = 2 * steps

    dims = [("tm", bit) for bit in bits_of(segments)[1:]]
    dims += [("batch", bit) for bit in bits_of(lax.axis_size("batch"))]
    turn = min(COLORS, len(dims))
    orders = [dims[i % turn : turn] + dims[: i % turn] + dims[turn:] for i in range(COLORS)]
    blocks = 1 << len(dims)
    used = (2 * width * hidden + hidden + width) // LANES
    block_rows = 8 * (-(-used // (8 * blocks * COLORS)))
    color_rows = blocks * block_rows
    packed_rows = COLORS * color_rows

    def position(order):
        place = jnp.int32(0)
        for axis, bit in order:
            index = segment if axis == "tm" else group
            place = 2 * place + (index // bit) % 2
        return place

    info = jnp.stack([core, stage] + [position(order) for order in orders]).astype(jnp.int32)

    def other_half(array):
        return lax.dynamic_slice_in_dim(array, (1 - core) * rows, rows, 1)

    mate_noise = flipped(other_half(increments), "tm", 1)
    mate_cotangent = flipped(other_half(cotangents), "tm", 1)
    weights = (
        drift_inner,
        drift_hidden.reshape(1, hidden),
        drift_outer,
        drift_offset.reshape(1, width),
        noise_inner,
        noise_hidden.reshape(1, hidden),
        noise_outer,
        noise_offset.reshape(1, width),
    )
    turned = (drift_inner.T, drift_outer.T, noise_inner.T, noise_outer.T)

    tiles = hidden // TILE
    weight_scratch = (
        pltpu.SemaphoreType.DMA,
        pltpu.VMEM((2, tiles, width, TILE), bf16),
        pltpu.VMEM((2, hidden, width), bf16),
    )

    def sds(shape, dtype=f32):
        return jax.ShapeDtypeStruct(shape, dtype)

    def forward(incoming, turn, full):
        out_shape = [sds((rows, width))]
        out_specs = [VMEM]
        scratch = [
            pltpu.VMEM((window, rows, width), f32),
            pltpu.SemaphoreType.DMA((window,)),
            *weight_scratch,
        ]
        if full:
            out_shape += [
                sds((steps, local_rows, width)),
                sds((steps, rows, width)),
                sds((window, rows, width), bf16),
                sds((tiles, window, rows, TILE), bf16),
                sds((tiles, window, rows, TILE), bf16),
                sds((window, rows, width)),
            ]
            out_specs += [ANY] * 6
            scratch += [
                pltpu.SemaphoreType.DMA,
                pltpu.VMEM((window, rows, width), f32),
                pltpu.VMEM((window, rows, width), bf16),
                pltpu.VMEM((tiles, window, rows, TILE), bf16),
                pltpu.VMEM((tiles, window, rows, TILE), bf16),
                pltpu.VMEM((window, rows, width), f32),
            ]
        return pl.pallas_call(
            functools.partial(forward_kernel, turn, full, steps, rows),
            out_shape=out_shape,
            in_specs=[SMEM, ANY if turn == 0 else VMEM, ANY, ANY]
            + [ANY, VMEM] * 4
            + [VMEM] * (turn > 0),
            out_specs=out_specs,
            scratch_shapes=scratch,
            compiler_params=PARAMS,
            name="forward_full" if full else "forward_light",
        )(info, initial_state, increments, mate_noise, *weights, *incoming)

    def relay(run, distance, reached):
        incoming = ()
        for turn in range(stages - 1):
            arrived = moved(run(incoming, turn, False)[0], distance)
            if turn > 0:
                arrived = jnp.where(reached == turn + 1, arrived, incoming[0])
            incoming = (arrived,)
        return run(incoming, stages - 1, True)

    unused, states, states_send, q, u, v, a = relay(forward, 2, stage)
    states_mate = flipped(states_send, "tm", 1)

    def backward(incoming, turn, full):
        out_shape = [sds((rows, width))]
        out_specs = [VMEM]
        scratch = [
            pltpu.VMEM((window, rows, width), f32),
            pltpu.VMEM((tiles, window, rows, TILE), bf16),
            pltpu.VMEM((tiles, window, rows, TILE), bf16),
            pltpu.VMEM((window, rows, width), f32),
            pltpu.SemaphoreType.DMA((window,)),
            *weight_scratch,
        ]
        if full:
            out_shape += [
                sds((steps, local_rows, width)),
                sds((steps, rows, width)),
                sds((packed_rows, LANES)),
                sds((packed_rows, LANES)),
            ]
            out_specs += [ANY] * 4
            scratch += [
                pltpu.SemaphoreType.DMA,
                pltpu.VMEM((window, rows, width), bf16),
                pltpu.VMEM((window, rows, width), f32),
                pltpu.VMEM((tiles, window, rows, TILE), bf16),
                pltpu.VMEM((tiles, window, rows, TILE), bf16),
                pltpu.VMEM((window * rows // TILE, width, TILE), bf16),
                pltpu.VMEM((window * rows // TILE, width, TILE), bf16),
                pltpu.VMEM((window * rows // TILE, width, TILE), bf16),
                pltpu.VMEM((8, hidden), f32),
                pltpu.VMEM((8, hidden), f32),
                pltpu.VMEM((8, width), f32),
                pltpu.VMEM((8, width), f32),
                pltpu.VMEM((2, packed_rows, LANES), f32),
            ]
        return pl.pallas_call(
            functools.partial(
                backward_kernel, turn, stages, full, steps, rows, blocks, block_rows
            ),
            out_shape=out_shape,
            in_specs=[SMEM] + [ANY] * 10 + [VMEM] * (turn > 0),
            out_specs=out_specs,
            scratch_shapes=scratch,
            compiler_params=PARAMS,
            name="backward_full" if full else "backward_light",
        )(info, cotangents, mate_cotangent, q, u, v, a, *turned, *incoming)

    unused, adjoints, adjoints_send, keep, send = relay(backward, -2, stages - 1 - stage)
    mate_grads = flipped(send, "tm", 1)
    adjoints_mate = flipped(adjoints_send, "tm", 1)

    parts = [[keep, mate_grads] for order in orders]
    starts = [[i * color_rows] * 2 for i in range(COLORS)]
    size = color_rows

    def gathered(i, begin, count):
        total = None
        for part, start in zip(parts[i], starts[i]):
            piece = part[start + begin : start + begin + count]
            total = piece if total is None else total + piece
        return total

    for phase in range(len(dims)):
        size //= 2
        arrived = [flipped(gathered(i, 0, size), *orders[i][phase]) for i in range(COLORS)]
        for i in range(COLORS):
            starts[i] = [start + size for start in starts[i]] + [0]
            parts[i].append(arrived[i])
    current = [gathered(i, 0, size) for i in range(COLORS)]
    for phase in reversed(range(1, len(dims))):
        arrived = [flipped(current[i], *orders[i][phase]) for i in range(COLORS)]
        current = [jnp.concatenate([arrived[i], current[i]], 0) for i in range(COLORS)]
    low_mate = [flipped(current[i], "tm", 1) for i in range(COLORS)]
    top = [flipped(current[i], *orders[i][0]) for i in range(COLORS)]
    top_mate = [flipped(top[i], "tm", 1) for i in range(COLORS)]
    pieces = []
    for i in range(COLORS):
        pieces += [current[i], top[i], low_mate[i], top_mate[i]]

    limit = 0.5 * math.sqrt(4 * width * hidden + 2 * hidden + 2 * width)
    shapes = [(width, hidden), (1, hidden), (hidden, width), (1, width)] * 2
    grads = pl.pallas_call(
        functools.partial(finish_kernel, blocks, block_rows, width, hidden, limit),
        out_shape=[sds(shape) for shape in shapes],
        in_specs=[SMEM] + [ANY] * len(pieces),
        out_specs=[VMEM] * 8,
        scratch_shapes=[
            pltpu.VMEM((2, packed_rows, LANES), f32),
            pltpu.SemaphoreType.DMA,
        ],
        compiler_params=PARAMS,
        name="finish",
    )(info, *pieces)
    grads = [g.reshape(-1) if g.shape[0] == 1 else g for g in grads]
    far = (1 - core) * rows
    states = lax.dynamic_update_slice_in_dim(states, states_mate, far, 1)
    adjoints = lax.dynamic_update_slice_in_dim(adjoints, adjoints_mate, far, 1)
    return (states, adjoints, *grads)


def solution(mesh):
    placed = (P("batch", None), P("tm", "batch", None), P("tm", "batch", None)) + (P(),) * 8
    return jax.shard_map(
        shards,
        mesh=mesh,
        in_specs=placed,
        out_specs=(P("tm", "batch", None), P("tm", "batch", None)) + (P(),) * 8,
        check_vma=False,
    )
```
